32 devices in a mesh: fs: 4 (over z), pp: 2 (over y), ep: 4 (over x, core).
Axes of the slice: x: 2, y: 2, z: 4, core: 2. Of those that a mesh axis runs over, the one named last changes fastest.
Arguments:
- w_gate: bfloat16 [2, 96, 1024, 512], P('pp', 'ep', None, 'fs')
- w_up: bfloat16 [2, 96, 1024, 512], P('pp', 'ep', None, 'fs')
- w_down: bfloat16 [2, 96, 512, 1024], P('pp', 'ep', 'fs')
- hot_ids: int32 [6], replicated
Outputs:
- output 1: bfloat16 [2, 96, 1024, 1024], P(None, ('pp', 'ep', 'fs'))
- output 2: bfloat16 [2, 96, 512, 1024], P(None, ('pp', 'ep', 'fs'))
- output 3: bfloat16 [2, 6, 1024, 1024], replicated
- output 4: bfloat16 [2, 6, 512, 1024], replicated
All inputs are finite; a program needn't handle non-finite values.
Results may differ from the reference program's by a relative error of at most 0.001.
Values are sent between devices in bfloat16 or wider.
A program may use at most 1 GiB of HBM per device.

```python
import jax
import jax.numpy as jnp

LAYERS = 2
EXPERTS = 96
D_MODEL = 1024
F_EXPERT = 512
HOT_COUNT = 6


def setup_inputs(seed: int = 0) -> dict:
    root_key = jax.random.key(seed)
    k_gate, k_up, k_down, k_hot = jax.random.split(root_key, 4)
    shape_in = (LAYERS, EXPERTS, D_MODEL, F_EXPERT)
    shape_down = (LAYERS, EXPERTS, F_EXPERT, D_MODEL)
    w_gate = (jax.random.normal(k_gate, shape_in, jnp.float32) * D_MODEL ** -0.5).astype(jnp.bfloat16)
    w_up = (jax.random.normal(k_up, shape_in, jnp.float32) * D_MODEL ** -0.5).astype(jnp.bfloat16)
    w_down = (jax.random.normal(k_down, shape_down, jnp.float32) * F_EXPERT ** -0.5).astype(jnp.bfloat16)
    hot_ids = jax.random.permutation(k_hot, EXPERTS)[:HOT_COUNT].astype(jnp.int32)
    return {"w_gate": w_gate, "w_up": w_up, "w_down": w_down, "hot_ids": hot_ids}


def reference(w_gate, w_up, w_down, hot_ids):
    gate_up = jnp.concatenate([w_gate, w_up], axis=-1)
    hot_gate_up = jnp.take(gate_up, hot_ids, axis=1)
    hot_down = jnp.take(w_down, hot_ids, axis=1)
    return gate_up, w_down, hot_gate_up, hot_down
```

```python
import functools

import jax
import jax.numpy as jnp
from jax import lax
from jax.experimental import pallas as pl
from jax.experimental.pallas import tpu as pltpu
from jax.sharding import PartitionSpec as P

ANY = pl.BlockSpec(memory_space=pl.ANY)
MESH = pl.DeviceIdType.MESH
FS, PP, EP = 4, 2, 4
N_T = 3


def pick_body(off_ref, gate_in, up_in, down_in, gate_out, up_out, down_out):
    gate_out[...] = gate_in[0]
    up_out[...] = up_in[0]
    down_out[...] = down_in[0]


def pick(w_gate, w_up, w_down, offset):
    hot = offset.shape[0]
    d, f = w_gate.shape[2:]
    src = lambda a, b: pl.BlockSpec((1, 1, a, b), lambda h, off: (0, off[h], 0, 0))
    dst = lambda a, b: pl.BlockSpec((1, a, b), lambda h, off: (h, 0, 0))
    return pl.pallas_call(
        pick_body,
        out_shape=(
            jax.ShapeDtypeStruct((hot, d, f), w_gate.dtype),
            jax.ShapeDtypeStruct((hot, d, f), w_gate.dtype),
            jax.ShapeDtypeStruct((hot, f, d), w_gate.dtype),
        ),
        grid_spec=pltpu.PrefetchScalarGridSpec(
            num_scalar_prefetch=1,
            grid=(hot,),
            in_specs=[src(d, f), src(d, f), src(f, d)],
            out_specs=[dst(d, f), dst(d, f), dst(f, d)],
        ),
        name="pick",
    )(offset, w_gate, w_up, w_down)


def exchange_body(
    exp_per_ep, ids, gate, up, down, hot_g, hot_u, hot_d, w13, w2, hot13, hot2,
    cand_g, cand_u, cand_d, sel_g, sel_u, sel_d,
    main_s, main_r, rs_s, rs_r, loc, own, z_s, z_r, x_s, x_r, y_s, y_r, p_s, p_r, da_s, da_r, db_s, db_r, px_s, px_r, py_s, py_r, pa_s, pa_r, pb_s, pb_r,
):
    z, p, e = lax.axis_index("fs"), lax.axis_index("pp"), lax.axis_index("ep")
    x, c = e // 2, lax.rem(e, 2)
    width = gate.shape[3]
    hot = hot_g.shape[0]
    cut_g, cut_d = hot_g.shape[1] // EP, hot_d.shape[1] // EP
    full = gate.shape[3] * FS

    def remote(s, d, ss, rs, to):
        return pltpu.make_async_remote_copy(s, d, ss, rs, device_id=to, device_id_type=MESH)

    def landed(d, rs):
        pltpu.make_async_copy(d, d, rs).wait()

    def home(lay, zz):
        col = pl.multiple_of(zz * width, width)
        return (
            w13.at[lay, :, :, pl.ds(col, width)],
            w13.at[lay, :, :, pl.ds(pl.multiple_of(full + col, width), width)],
            w2.at[lay, :, pl.ds(col, width), :],
        )

    def main_to(zz, b):
        return (zz, x, lax.rem(2 * e + b, EP))

    def main_is_self(zz, b):
        return jnp.logical_and(jnp.logical_and(x == p, lax.rem(2 * e + b, EP) == e), zz == z)

    def main_copies(zz, b):
        k = b * FS + zz
        src = pl.ds(3 * k, 3)
        return [(a.at[0, src], d, k * N_T + t) for t, (a, d) in enumerate(zip((gate, up, down), home(p, z)))]

    def main_start(zz, b):
        mine = main_is_self(zz, b)

        @pl.when(jnp.logical_not(mine))
        def _():
            for s, d, i in main_copies(zz, b):
                remote(s, d, main_s.at[i], main_r.at[(p * FS + z) * N_T + lax.rem(i, N_T)], main_to(zz, b)).start()

        @pl.when(mine)
        def _():
            for t, (s, d, i) in enumerate(main_copies(zz, b)):
                pltpu.make_async_copy(s, d, loc.at[t]).start()

    def main_sent(zz, b):
        mine = main_is_self(zz, b)

        @pl.when(jnp.logical_not(mine))
        def _():
            for s, d, i in main_copies(zz, b):
                remote(s, d, main_s.at[i], main_s.at[i], main_to(zz, b)).wait_send()

        @pl.when(mine)
        def _():
            for t, (s, d, i) in enumerate(main_copies(zz, b)):
                pltpu.make_async_copy(s, d, loc.at[t]).wait()

    def main_landed(ys, zs):
        mine = jnp.logical_and(jnp.logical_and(2 * p + x == e, p == ys), z == zs)

        @pl.when(jnp.logical_not(mine))
        def _():
            for t, d in enumerate(home(ys, zs)):
                landed(d, main_r.at[(ys * FS + zs) * N_T + t])

    def piece(yy, q, zz, lo=0, hi=hot):
        col = pl.multiple_of(zz * width, width)
        rows = pl.ds(pl.multiple_of(q * cut_g, cut_g), cut_g)
        slots = pl.ds(lo, hi - lo)
        return (
            hot13.at[yy, slots, rows, pl.ds(col, width)],
            hot13.at[yy, slots, rows, pl.ds(pl.multiple_of(full + col, width), width)],
            hot2.at[yy, slots, pl.ds(pl.multiple_of(col + q * cut_d, cut_d), cut_d), :],
        )

    half = hot // 2
    q_x, q_p = 2 * (1 - x) + c, 2 * x + (1 - c)
    to_x, to_y, to_p = (z, p, q_x), (z, 1 - p, e), (z, p, q_p)

    def send(src, dst, ss, rs, i, to):
        for t in range(N_T):
            remote(src[t], dst[t], ss.at[i * N_T + t], rs.at[i * N_T + t], to).start()

    def sent(src, ss, i, to):
        for t in range(N_T):
            remote(src[t], src[t], ss.at[i * N_T + t], ss.at[i * N_T + t], to).wait_send()

    def arrived(dst, rs, i):
        for t in range(N_T):
            landed(dst[t], rs.at[i * N_T + t])

    def part(q):
        return (
            hot_g.at[:, pl.ds(pl.multiple_of(q * cut_g, cut_g), cut_g), :],
            hot_u.at[:, pl.ds(pl.multiple_of(q * cut_g, cut_g), cut_g), :],
            hot_d.at[:, pl.ds(pl.multiple_of(q * cut_d, cut_d), cut_d), :],
        )

    def cand(q):
        return cand_g.at[q], cand_u.at[q], cand_d.at[q]

    for k in range(1, EP):
        q = lax.rem(e + k, EP)
        for t in range(N_T):
            remote(part(q)[t], cand(e)[t], rs_s.at[k * N_T + t], rs_r.at[k * N_T + t], (z, p, q)).start()
    for t in range(N_T):
        pltpu.make_async_copy(part(e)[t], cand(e)[t], own.at[t]).start()

    order = [(kk, b) for kk in (2, 1, 3, 0) for b in range(2)]
    for kk, b in order:
        main_start(lax.rem(z + kk, FS), b)

    for t in range(N_T):
        pltpu.make_async_copy(part(e)[t], cand(e)[t], own.at[t]).wait()
    for k in range(1, EP):
        q = lax.rem(e + EP - k, EP)
        for t in range(N_T):
            landed(cand(q)[t], rs_r.at[k * N_T + t])

    for h in range(hot):
        holder = ids[h] // exp_per_ep
        sel_g[h] = cand_g[holder, h]
        sel_u[h] = cand_u[holder, h]
        sel_d[h] = cand_d[holder, h]
    sel = (sel_g, sel_u, sel_d)

    def broadcast(src, zz, k):
        dst = piece(p, e, zz)
        send(src, dst, x_s, x_r, k, to_x)
        send(src, dst, y_s, y_r, k, to_y)
        send(src, dst, p_s, p_r, k, to_p)

    mine = piece(p, e, z)
    UP, DOWN = 0, 1

    @pl.when(z < FS - 1)
    def _():
        send(sel, mine, z_s, z_r, UP * FS + 1, (z + 1, p, e))

    @pl.when(z > 0)
    def _():
        send(sel, mine, z_s, z_r, DOWN * FS + 1, (z - 1, p, e))

    broadcast(sel, z, z)
    for t in range(N_T):
        pltpu.make_async_copy(sel[t], mine[t], own.at[t]).start()

    def z_step(k):
        @pl.when(z - k >= 0)
        def _():
            src = piece(p, e, z - k)
            arrived(src, z_r, UP * FS + k)

            @pl.when(z < FS - 1)
            def _():
                send(src, src, z_s, z_r, UP * FS + k + 1, (z + 1, p, e))

            broadcast(src, z - k, z - k)

        @pl.when(z + k < FS)
        def _():
            src = piece(p, e, z + k)
            arrived(src, z_r, DOWN * FS + k)

            @pl.when(z > 0)
            def _():
                send(src, src, z_s, z_r, DOWN * FS + k + 1, (z - 1, p, e))

            broadcast(src, z + k, z + k)

    def plane_step(zz):
        from_x = piece(p, q_x, zz)
        arrived(from_x, x_r, zz)
        a = piece(p, q_x, zz, 0, half)
        send(a, a, da_s, da_r, zz, to_y)
        send(from_x, from_x, px_s, px_r, zz, to_p)
        from_y = piece(1 - p, e, zz)
        arrived(from_y, y_r, zz)
        b = piece(1 - p, e, zz, half, hot)
        send(b, b, db_s, db_r, zz, to_x)
        send(from_y, from_y, py_s, py_r, zz, to_p)

    def diagonal_step(zz):
        a = piece(1 - p, q_x, zz, 0, half)
        arrived(a, da_r, zz)
        send(a, a, pa_s, pa_r, zz, to_p)
        b = piece(1 - p, q_x, zz, half, hot)
        arrived(b, db_r, zz)
        send(b, b, pb_s, pb_r, zz, to_p)

    for k in range(1, FS):
        z_step(k)
    for k in range(FS):
        plane_step(lax.rem(z + k, FS))
    for k in range(FS):
        diagonal_step(lax.rem(z + k, FS))

    for t in range(N_T):
        pltpu.make_async_copy(sel[t], mine[t], own.at[t]).wait()
    for k in range(1, EP):
        q = lax.rem(e + k, EP)
        for t in range(N_T):
            remote(part(q)[t], cand(e)[t], rs_s.at[k * N_T + t], rs_s.at[k * N_T + t], (z, p, q)).wait_send()
    for k in range(1, FS):
        @pl.when(jnp.logical_and(z - k + 1 >= 0, z < FS - 1))
        def _():
            sent(mine, z_s, UP * FS + k, (z + 1, p, e))

        @pl.when(jnp.logical_and(z + k - 1 < FS, z > 0))
        def _():
            sent(mine, z_s, DOWN * FS + k, (z - 1, p, e))
    for zz in range(FS):
        src = piece(p, e, zz)
        sent(src, x_s, zz, to_x)
        sent(src, y_s, zz, to_y)
        sent(src, p_s, zz, to_p)
        sent(src, px_s, zz, to_p)
        sent(src, py_s, zz, to_p)
        a = piece(p, q_x, zz, 0, half)
        sent(a, da_s, zz, to_y)
        sent(a, db_s, zz, to_x)
        sent(a, pa_s, zz, to_p)
        sent(a, pb_s, zz, to_p)
        q_px = 2 * (1 - x) + (1 - c)
        arrived(piece(p, q_p, zz), p_r, zz)
        arrived(piece(p, q_px, zz), px_r, zz)
        arrived(piece(1 - p, q_p, zz), py_r, zz)
        arrived(piece(1 - p, q_px, zz, 0, half), pa_r, zz)
        arrived(piece(1 - p, q_px, zz, half, hot), pb_r, zz)
    for kk, b in order:
        main_sent(lax.rem(z + kk, FS), b)
    for ys in range(PP):
        for zs in range(FS):
            main_landed(ys, zs)


def exchange(ids, w_gate, w_up, w_down, hot_g, hot_u, hot_d):
    dt = w_gate.dtype
    exp_local, d, f = w_gate.shape[1:]
    hot = hot_g.shape[0]
    per_dev = exp_local // (FS * PP)
    full = f * FS
    dma = lambda n: pltpu.SemaphoreType.DMA((n,))
    quarter = [(hot, d // EP, f), (hot, d // EP, f), (hot, f // EP, d)]
    four = lambda: [dma(FS * N_T), dma(FS * N_T)]
    return pl.pallas_call(
        functools.partial(exchange_body, exp_local),
        out_shape=(
            jax.ShapeDtypeStruct((PP, per_dev, d, 2 * full), dt),
            jax.ShapeDtypeStruct((PP, per_dev, full, d), dt),
            jax.ShapeDtypeStruct((PP, hot, d, 2 * full), dt),
            jax.ShapeDtypeStruct((PP, hot, full, d), dt),
        ),
        in_specs=[pl.BlockSpec(memory_space=pltpu.SMEM)] + [ANY] * 6,
        out_specs=(ANY,) * 4,
        scratch_shapes=[pltpu.VMEM((EP,) + s, dt) for s in quarter]
        + [pltpu.VMEM(s, dt) for s in quarter]
        + [dma(FS * PP * N_T), dma(FS * PP * N_T), dma(EP * N_T), dma(EP * N_T), dma(N_T), dma(N_T)]
        + [dma(2 * FS * N_T), dma(2 * FS * N_T)]
        + four() * 9,
        compiler_params=pltpu.CompilerParams(has_side_effects=True),
        name="exchange",
    )(ids, w_gate, w_up, w_down, hot_g, hot_u, hot_d)


def solution(mesh):
    in_spec = P("pp", "ep", None, "fs")
    down_spec = P("pp", "ep", "fs", None)
    home_spec = P(None, ("pp", "ep", "fs"), None, None)

    def device_body(w_gate, w_up, w_down, hot_ids):
        exp_local = w_gate.shape[1]
        offset = jnp.clip(hot_ids - lax.axis_index("ep") * exp_local, 0, exp_local - 1)
        picked = pick(w_gate, w_up, w_down, offset)
        return exchange(hot_ids, w_gate, w_up, w_down, *picked)

    return jax.shard_map(
        device_body,
        mesh=mesh,
        in_specs=(in_spec, in_spec, down_spec, P()),
        out_specs=(home_spec, home_spec, P(), P()),
        check_vma=False,
    )
```

```python
import functools

import jax
import jax.numpy as jnp
from jax import lax
from jax.experimental import pallas as pl
from jax.experimental.pallas import tpu as pltpu
from jax.sharding import PartitionSpec as P

ANY = pl.BlockSpec(memory_space=pl.ANY)
MESH = pl.DeviceIdType.MESH
FS, PP, EP = 4, 2, 4
N_T = 3
LATE = 2
ORDER = [(kk, b, t) for t in range(N_T) for b in range(2) for kk in (1, 3, 2, 0) if (kk, b, t) != (LATE, 1, 2)]
BATCH = (8, 0, 0, 0, 0)


def pick_body(off_ref, gate_in, up_in, down_in, gate_out, up_out, down_out):
    gate_out[...] = gate_in[0]
    up_out[...] = up_in[0]
    down_out[...] = down_in[0]


def pick(w_gate, w_up, w_down, offset):
    hot = offset.shape[0]
    d, f = w_gate.shape[2:]
    src = lambda a, b: pl.BlockSpec((1, 1, a, b), lambda h, off: (0, off[h], 0, 0))
    dst = lambda a, b: pl.BlockSpec((1, a, b), lambda h, off: (h, 0, 0))
    return pl.pallas_call(
        pick_body,
        out_shape=(
            jax.ShapeDtypeStruct((hot, d, f), w_gate.dtype),
            jax.ShapeDtypeStruct((hot, d, f), w_gate.dtype),
            jax.ShapeDtypeStruct((hot, f, d), w_gate.dtype),
        ),
        grid_spec=pltpu.PrefetchScalarGridSpec(
            num_scalar_prefetch=1,
            grid=(hot,),
            in_specs=[src(d, f), src(d, f), src(f, d)],
            out_specs=[dst(d, f), dst(d, f), dst(f, d)],
        ),
        name="pick",
    )(offset, w_gate, w_up, w_down)


def exchange_body(
    exp_per_ep, ids, gate, up, down, hot_g, hot_u, hot_d, w13, w2, hot13, hot2, late,
    cand_g, cand_u, cand_d, sel_g, sel_u, sel_d,
    main_s, main_r, rs_s, rs_r, loc, own, z_s, z_r, x_s, x_r, y_s, y_r, p_s, p_r, da_s, da_r, db_s, db_r, px_s, px_r, py_s, py_r, pa_s, pa_r, pb_s, pb_r,
):
    z, p, e = lax.axis_index("fs"), lax.axis_index("pp"), lax.axis_index("ep")
    x, c = e // 2, lax.rem(e, 2)
    width = gate.shape[3]
    hot = hot_g.shape[0]
    cut_g, cut_d = hot_g.shape[1] // EP, hot_d.shape[1] // EP
    full = gate.shape[3] * FS

    def remote(s, d, ss, rs, to):
        return pltpu.make_async_remote_copy(s, d, ss, rs, device_id=to, device_id_type=MESH)

    def landed(d, rs):
        pltpu.make_async_copy(d, d, rs).wait()

    def home(lay, zz):
        col = pl.multiple_of(zz * width, width)
        return (
            w13.at[lay, :, :, pl.ds(col, width)],
            w13.at[lay, :, :, pl.ds(pl.multiple_of(full + col, width), width)],
            w2.at[lay, :, pl.ds(col, width), :],
        )

    def main_to(zz, b):
        return (zz, x, lax.rem(2 * e + b, EP))

    def main_is_self(zz, b):
        return jnp.logical_and(jnp.logical_and(x == p, lax.rem(2 * e + b, EP) == e), zz == z)

    def main_copy(zz, b, t):
        k = b * FS + zz
        return (gate, up, down)[t].at[0, pl.ds(3 * k, 3)], home(p, z)[t], k * N_T + t

    def main_start(zz, b, t):
        mine = main_is_self(zz, b)
        s, d, i = main_copy(zz, b, t)

        @pl.when(jnp.logical_not(mine))
        def _():
            remote(s, d, main_s.at[i], main_r.at[(p * FS + z) * N_T + t], main_to(zz, b)).start()

        @pl.when(mine)
        def _():
            pltpu.make_async_copy(s, d, loc.at[t]).start()

    def main_sent(zz, b, t):
        mine = main_is_self(zz, b)
        s, d, i = main_copy(zz, b, t)

        @pl.when(jnp.logical_not(mine))
        def _():
            remote(s, d, main_s.at[i], main_s.at[i], main_to(zz, b)).wait_send()

        @pl.when(mine)
        def _():
            pltpu.make_async_copy(s, d, loc.at[t]).wait()

    queue = [(lax.rem(z + kk, FS), 1 - p if (kk, t) == (LATE, 2) else b, t) for kk, b, t in ORDER]
    late_src = down.at[0, pl.ds(3 * (p * FS + lax.rem(z + LATE, FS)), 3)]
    pltpu.make_async_copy(late_src, late, loc.at[N_T]).start()
    started = []

    def main_next(n):
        for item in queue[len(started) : len(started) + n]:
            main_start(*item)
            started.append(item)

    def main_landed(ys, zs):
        mine = jnp.logical_and(jnp.logical_and(2 * p + x == e, p == ys), z == zs)

        is_late = jnp.logical_and(ys == c, zs == lax.rem(z + LATE, FS))
        for t, d in enumerate(home(ys, zs)):
            skip = jnp.logical_or(mine, is_late) if t == 2 else mine

            @pl.when(jnp.logical_not(skip))
            def _():
                landed(d, main_r.at[(ys * FS + zs) * N_T + t])

    def piece(yy, q, zz, lo=0, hi=hot):
        col = pl.multiple_of(zz * width, width)
        rows = pl.ds(pl.multiple_of(q * cut_g, cut_g), cut_g)
        slots = pl.ds(lo, hi - lo)
        return (
            hot13.at[yy, slots, rows, pl.ds(col, width)],
            hot13.at[yy, slots, rows, pl.ds(pl.multiple_of(full + col, width), width)],
            hot2.at[yy, slots, pl.ds(pl.multiple_of(col + q * cut_d, cut_d), cut_d), :],
        )

    half = hot // 2
    q_x, q_p = 2 * (1 - x) + c, 2 * x + (1 - c)
    to_x, to_y, to_p = (z, p, q_x), (z, 1 - p, e), (z, p, q_p)

    def send(src, dst, ss, rs, i, to):
        for t in range(N_T):
            remote(src[t], dst[t], ss.at[i * N_T + t], rs.at[i * N_T + t], to).start()

    def sent(src, ss, i, to):
        for t in range(N_T):
            remote(src[t], src[t], ss.at[i * N_T + t], ss.at[i * N_T + t], to).wait_send()

    def arrived(dst, rs, i):
        for t in range(N_T):
            landed(dst[t], rs.at[i * N_T + t])

    def part(q):
        return (
            hot_g.at[:, pl.ds(pl.multiple_of(q * cut_g, cut_g), cut_g), :],
            hot_u.at[:, pl.ds(pl.multiple_of(q * cut_g, cut_g), cut_g), :],
            hot_d.at[:, pl.ds(pl.multiple_of(q * cut_d, cut_d), cut_d), :],
        )

    def cand(q):
        return cand_g.at[q], cand_u.at[q], cand_d.at[q]

    for k in range(1, EP):
        q = lax.rem(e + k, EP)
        for t in range(N_T):
            remote(part(q)[t], cand(e)[t], rs_s.at[k * N_T + t], rs_r.at[k * N_T + t], (z, p, q)).start()
    for t in range(N_T):
        pltpu.make_async_copy(part(e)[t], cand(e)[t], own.at[t]).start()

    main_next(BATCH[0])

    for t in range(N_T):
        pltpu.make_async_copy(part(e)[t], cand(e)[t], own.at[t]).wait()
    for k in range(1, EP):
        q = lax.rem(e + EP - k, EP)
        for t in range(N_T):
            landed(cand(q)[t], rs_r.at[k * N_T + t])

    for h in range(hot):
        holder = ids[h] // exp_per_ep
        sel_g[h] = cand_g[holder, h]
        sel_u[h] = cand_u[holder, h]
        sel_d[h] = cand_d[holder, h]
    sel = (sel_g, sel_u, sel_d)

    def broadcast(src, zz, k):
        dst = piece(p, e, zz)
        send(src, dst, x_s, x_r, k, to_x)
        send(src, dst, y_s, y_r, k, to_y)
        send(src, dst, p_s, p_r, k, to_p)

    mine = piece(p, e, z)
    UP, DOWN = 0, 1

    @pl.when(z < FS - 1)
    def _():
        send(sel, mine, z_s, z_r, UP * FS + 1, (z + 1, p, e))

    @pl.when(z > 0)
    def _():
        send(sel, mine, z_s, z_r, DOWN * FS + 1, (z - 1, p, e))

    main_next(BATCH[1])
    broadcast(sel, z, z)
    for t in range(N_T):
        pltpu.make_async_copy(sel[t], mine[t], own.at[t]).start()

    def z_step(k):
        @pl.when(z - k >= 0)
        def _():
            src = piece(p, e, z - k)
            arrived(src, z_r, UP * FS + k)

            @pl.when(z < FS - 1)
            def _():
                send(src, src, z_s, z_r, UP * FS + k + 1, (z + 1, p, e))

            broadcast(src, z - k, z - k)

        @pl.when(z + k < FS)
        def _():
            src = piece(p, e, z + k)
            arrived(src, z_r, DOWN * FS + k)

            @pl.when(z > 0)
            def _():
                send(src, src, z_s, z_r, DOWN * FS + k + 1, (z - 1, p, e))

            broadcast(src, z + k, z + k)

    def plane_step(zz):
        from_x = piece(p, q_x, zz)
        arrived(from_x, x_r, zz)
        a = piece(p, q_x, zz, 0, half)
        send(a, a, da_s, da_r, zz, to_y)
        send(from_x, from_x, px_s, px_r, zz, to_p)
        from_y = piece(1 - p, e, zz)
        arrived(from_y, y_r, zz)
        b = piece(1 - p, e, zz, half, hot)
        send(b, b, db_s, db_r, zz, to_x)
        send(from_y, from_y, py_s, py_r, zz, to_p)

    def diagonal_step(zz):
        a = piece(1 - p, q_x, zz, 0, half)
        arrived(a, da_r, zz)
        send(a, a, pa_s, pa_r, zz, to_p)
        b = piece(1 - p, q_x, zz, half, hot)
        arrived(b, db_r, zz)
        send(b, b, pb_s, pb_r, zz, to_p)

    for k in range(1, FS):
        z_step(k)
        main_next(BATCH[1 + k])
    main_next(len(queue))
    for k in range(FS):
        plane_step(lax.rem(z + k, FS))
    for k in range(FS):
        diagonal_step(lax.rem(z + k, FS))

    for t in range(N_T):
        pltpu.make_async_copy(sel[t], mine[t], own.at[t]).wait()
    for k in range(1, EP):
        q = lax.rem(e + k, EP)
        for t in range(N_T):
            remote(part(q)[t], cand(e)[t], rs_s.at[k * N_T + t], rs_s.at[k * N_T + t], (z, p, q)).wait_send()
    for k in range(1, FS):
        @pl.when(jnp.logical_and(z - k + 1 >= 0, z < FS - 1))
        def _():
            sent(mine, z_s, UP * FS + k, (z + 1, p, e))

        @pl.when(jnp.logical_and(z + k - 1 < FS, z > 0))
        def _():
            sent(mine, z_s, DOWN * FS + k, (z - 1, p, e))
    for zz in range(FS):
        src = piece(p, e, zz)
        sent(src, x_s, zz, to_x)
        sent(src, y_s, zz, to_y)
        sent(src, p_s, zz, to_p)
        sent(src, px_s, zz, to_p)
        sent(src, py_s, zz, to_p)
        a = piece(p, q_x, zz, 0, half)
        sent(a, da_s, zz, to_y)
        sent(a, db_s, zz, to_x)
        sent(a, pa_s, zz, to_p)
        sent(a, pb_s, zz, to_p)
        q_px = 2 * (1 - x) + (1 - c)
        arrived(piece(p, q_p, zz), p_r, zz)
        arrived(piece(p, q_px, zz), px_r, zz)
        arrived(piece(1 - p, q_p, zz), py_r, zz)
        arrived(piece(1 - p, q_px, zz, 0, half), pa_r, zz)
        arrived(piece(1 - p, q_px, zz, half, hot), pb_r, zz)
    for item in queue:
        main_sent(*item)
    pltpu.make_async_copy(late_src, late, loc.at[N_T]).wait()
    for ys in range(PP):
        for zs in range(FS):
            main_landed(ys, zs)


def exchange(ids, w_gate, w_up, w_down, hot_g, hot_u, hot_d):
    dt = w_gate.dtype
    exp_local, d, f = w_gate.shape[1:]
    hot = hot_g.shape[0]
    per_dev = exp_local // (FS * PP)
    full = f * FS
    dma = lambda n: pltpu.SemaphoreType.DMA((n,))
    quarter = [(hot, d // EP, f), (hot, d // EP, f), (hot, f // EP, d)]
    four = lambda: [dma(FS * N_T), dma(FS * N_T)]
    return pl.pallas_call(
        functools.partial(exchange_body, exp_local),
        out_shape=(
            jax.ShapeDtypeStruct((PP, per_dev, d, 2 * full), dt),
            jax.ShapeDtypeStruct((PP, per_dev, full, d), dt),
            jax.ShapeDtypeStruct((PP, hot, d, 2 * full), dt),
            jax.ShapeDtypeStruct((PP, hot, full, d), dt),
            jax.ShapeDtypeStruct((per_dev, f, d), dt),
        ),
        in_specs=[pl.BlockSpec(memory_space=pltpu.SMEM)] + [ANY] * 6,
        out_specs=(ANY,) * 5,
        scratch_shapes=[pltpu.VMEM((EP,) + s, dt) for s in quarter]
        + [pltpu.VMEM(s, dt) for s in quarter]
        + [dma(FS * PP * N_T), dma(FS * PP * N_T), dma(EP * N_T), dma(EP * N_T), dma(N_T + 1), dma(N_T)]
        + [dma(2 * FS * N_T), dma(2 * FS * N_T)]
        + four() * 9,
        compiler_params=pltpu.CompilerParams(has_side_effects=True),
        name="exchange",
    )(ids, w_gate, w_up, w_down, hot_g, hot_u, hot_d)


def settle_body(n_slot, ahead, *refs):
    n = (len(refs) - 3) // 2
    src, dst, (buf, r_sem, w_sem) = refs[:n], refs[n : 2 * n], refs[2 * n :]
    steps = [(a, i, j) for a in range(n) for i in range(src[a].shape[0]) for j in range(src[a].shape[1])]

    def load(k):
        a, i, j = steps[k]
        return pltpu.make_async_copy(src[a].at[i, j], buf.at[k % n_slot, pl.ds(0, src[a].shape[2])], r_sem.at[k % n_slot])

    def store(k):
        a, i, j = steps[k]
        return pltpu.make_async_copy(buf.at[k % n_slot, pl.ds(0, src[a].shape[2])], dst[a].at[i, j], w_sem.at[k % n_slot])

    for k in range(min(ahead, len(steps))):
        load(k).start()
    for k in range(len(steps)):
        load(k).wait()
        store(k).start()
        if k + ahead < len(steps):
            if k + ahead >= n_slot:
                store(k + ahead - n_slot).wait()
            load(k + ahead).start()
    for k in range(max(0, len(steps) - n_slot), len(steps)):
        store(k).wait()


def settle(*arrays):
    n_slot, ahead = 12, 6
    rows = max(a.shape[2] for a in arrays)
    size = sum(a.size * a.dtype.itemsize for a in arrays)
    return pl.pallas_call(
        functools.partial(settle_body, n_slot, ahead),
        out_shape=tuple(jax.ShapeDtypeStruct(a.shape, a.dtype) for a in arrays),
        in_specs=[ANY] * len(arrays),
        out_specs=(ANY,) * len(arrays),
        scratch_shapes=[
            pltpu.VMEM((n_slot, rows, arrays[0].shape[3]), arrays[0].dtype),
            pltpu.SemaphoreType.DMA((n_slot,)),
            pltpu.SemaphoreType.DMA((n_slot,)),
        ],
        cost_estimate=pl.CostEstimate(flops=size * 16, bytes_accessed=2 * size, transcendentals=0),
        name="settle",
    )(*arrays)


def insert_body(at_ref, piece_in, whole_in, whole_out):
    whole_out[0] = piece_in[...]


def insert(whole, piece, lay, zz):
    _, f, d = piece.shape
    return pl.pallas_call(
        insert_body,
        out_shape=jax.ShapeDtypeStruct(whole.shape, whole.dtype),
        grid_spec=pltpu.PrefetchScalarGridSpec(
            num_scalar_prefetch=1,
            grid=(piece.shape[0],),
            in_specs=[pl.BlockSpec((1, f, d), lambda h, at: (h, 0, 0)), ANY],
            out_specs=pl.BlockSpec((1, 1, f, d), lambda h, at: (at[0], h, at[1], 0)),
        ),
        input_output_aliases={2: 0},
        name="insert",
    )(jnp.stack([lay, zz]), piece, whole)


def late_pairs():
    flat = lambda z, p, e: (z * PP + p) * EP + e
    return [
        (flat(z, p, e), flat((z + LATE) % FS, e // 2, (2 * e + p) % EP))
        for z in range(FS)
        for p in range(PP)
        for e in range(EP)
    ]


def solution(mesh):
    in_spec = P("pp", "ep", None, "fs")
    down_spec = P("pp", "ep", "fs", None)
    home_spec = P(None, ("pp", "ep", "fs"), None, None)

    def device_body(w_gate, w_up, w_down, hot_ids):
        exp_local = w_gate.shape[1]
        offset = jnp.clip(hot_ids - lax.axis_index("ep") * exp_local, 0, exp_local - 1)
        picked = pick(w_gate, w_up, w_down, offset)
        *came, late = exchange(hot_ids, w_gate, w_up, w_down, *picked)
        late = lax.ppermute(late, ("fs", "pp", "ep"), late_pairs())
        w13, w2, hot13, hot2 = settle(*came)
        core, z = lax.rem(lax.axis_index("ep"), 2), lax.axis_index("fs")
        w2 = insert(w2, late, core, lax.rem(z + LATE, FS))
        return w13, w2, hot13, hot2

    return jax.shard_map(
        device_body,
        mesh=mesh,
        in_specs=(in_spec, in_spec, down_spec, P()),
        out_specs=(home_spec, home_spec, P(), P()),
        check_vma=False,
    )
```

```python
import functools

import jax
import jax.numpy as jnp
from jax import lax
from jax.experimental import pallas as pl
from jax.experimental.pallas import tpu as pltpu
from jax.sharding import PartitionSpec as P

ANY = pl.BlockSpec(memory_space=pl.ANY)
HBM = pl.BlockSpec(memory_space=pltpu.HBM)
VMEM = pl.BlockSpec(memory_space=pltpu.VMEM)
MESH = pl.DeviceIdType.MESH
FS, PP, EP = 4, 2, 4
N_T = 3
LATE = 2
OUTER = [(m, b, t) for t in range(N_T) for b in range(2) for m in (1, 3, 2, 0) if (m, b, t) != (2, 1, 2)]
INNER = [(m, b, t) for t in range(N_T) for b in range(2) for m in (2, 0, 3, 1) if (m, b, t) != (3, 1, 2)]
COUNTS = (6, 0, 0, 0, 24)


def in_hbm(a):
    return pltpu.with_memory_space_constraint(a, pltpu.HBM)


def in_vmem(a):
    return pltpu.with_memory_space_constraint(a, pltpu.VMEM)


def pick_body(exp_per_ep, ids, gate, up, down, gate_out, up_out, down_out, sems):
    base = lax.axis_index("ep") * exp_per_ep
    copies = []
    for h in range(gate_out.shape[0]):
        held = jnp.clip(ids[h] - base, 0, exp_per_ep - 1)
        for t, (s, d) in enumerate(((gate, gate_out), (up, up_out), (down, down_out))):
            copies.append(pltpu.make_async_copy(s.at[0, held], d.at[h], sems.at[h * N_T + t]))
    for copy in copies:
        copy.start()
    for copy in copies:
        copy.wait()


def pick(ids, w_gate, w_up, w_down):
    hot = ids.shape[0]
    exp_local, d, f = w_gate.shape[1:]
    dt = w_gate.dtype
    return pl.pallas_call(
        functools.partial(pick_body, exp_local),
        out_shape=(pltpu.VMEM((hot, d, f), dt), pltpu.VMEM((hot, d, f), dt), pltpu.VMEM((hot, f, d), dt)),
        in_specs=[pl.BlockSpec(memory_space=pltpu.SMEM)] + [HBM] * N_T,
        out_specs=(pl.BlockSpec(memory_space=pltpu.VMEM),) * N_T,
        scratch_shapes=[pltpu.SemaphoreType.DMA((hot * N_T,))],
        compiler_params=pltpu.CompilerParams(vmem_limit_bytes=4 << 20),
        name="pick",
    )(ids, w_gate, w_up, w_down)


def exchange_body(
    exp_per_ep, ids, gate, up, down, hot_g, hot_u, hot_d, w13, w2, hot13, hot2, late,
    got_g, got_u, got_d, got_xg, got_xu, got_xd, snd_g, snd_u, snd_d, keep_g, keep_u, keep_d, sel_g, sel_u, sel_d,
    main_s, main_r, rs_s, rs_r, loc, own, z_s, z_r, x_s, x_r, y_s, y_r, p_s, p_r, da_s, da_r, db_s, db_r, px_s, px_r, py_s, py_r, pa_s, pa_r, pb_s, pb_r,
):
    z, p, e = lax.axis_index("fs"), lax.axis_index("pp"), lax.axis_index("ep")
    x, c = e // 2, lax.rem(e, 2)
    width = gate.shape[3]
    hot = hot_g.shape[0]
    cut_g, cut_d = hot_g.shape[1] // EP, hot_d.shape[1] // EP
    full = gate.shape[3] * FS

    def remote(s, d, ss, rs, to):
        return pltpu.make_async_remote_copy(s, d, ss, rs, device_id=to, device_id_type=MESH)

    def landed(d, rs):
        pltpu.make_async_copy(d, d, rs).wait()

    def home(lay, zz):
        col = pl.multiple_of(zz * width, width)
        return (
            w13.at[lay, :, :, pl.ds(col, width)],
            w13.at[lay, :, :, pl.ds(pl.multiple_of(full + col, width), width)],
            w2.at[lay, :, pl.ds(col, width), :],
        )

    def main_to(zz, b):
        return (zz, x, lax.rem(2 * e + b, EP))

    def main_is_self(zz, b):
        return jnp.logical_and(jnp.logical_and(x == p, lax.rem(2 * e + b, EP) == e), zz == z)

    def main_copy(zz, b, t):
        k = b * FS + zz
        return (gate, up, down)[t].at[0, pl.ds(3 * k, 3)], home(p, z)[t], k * N_T + t

    def main_start(zz, b, t):
        mine = main_is_self(zz, b)
        s, d, i = main_copy(zz, b, t)

        @pl.when(jnp.logical_not(mine))
        def _():
            remote(s, d, main_s.at[i], main_r.at[(p * FS + z) * N_T + t], main_to(zz, b)).start()

        @pl.when(mine)
        def _():
            pltpu.make_async_copy(s, d, loc.at[t]).start()

    def main_sent(zz, b, t):
        mine = main_is_self(zz, b)
        s, d, i = main_copy(zz, b, t)

        @pl.when(jnp.logical_not(mine))
        def _():
            remote(s, d, main_s.at[i], main_s.at[i], main_to(zz, b)).wait_send()

        @pl.when(mine)
        def _():
            pltpu.make_async_copy(s, d, loc.at[t]).wait()

    upper = z // 2
    inner = z * (1 - upper) + (FS - 1 - z) * upper

    def group(items, late_plane):
        for m, b, t in items:
            b = 1 - p if t == 2 and m == late_plane else b
            main_start(m * (1 - upper) + (FS - 1 - m) * upper, b, t)

    bounds = [0]

    def after_step():
        lo = bounds[-1]
        step = len(bounds) - 1
        hi = min(len(OUTER), lo + (COUNTS[step] if step < len(COUNTS) else len(OUTER)))
        bounds.append(hi)
        if hi > lo:
            pl.when(inner == 0)(lambda: group(OUTER[lo:hi], LATE))
            pl.when(inner == 1)(lambda: group(INNER[lo:hi], LATE + 1))

    late_src = down.at[0, pl.ds(3 * (p * FS + lax.rem(z + LATE, FS)), 3)]
    pltpu.make_async_copy(late_src, late, loc.at[N_T]).start()
    def main_landed(ys, zs):
        mine = jnp.logical_and(jnp.logical_and(2 * p + x == e, p == ys), z == zs)

        is_late = jnp.logical_and(ys == c, zs == lax.rem(z + LATE, FS))
        for t, d in enumerate(home(ys, zs)):
            skip = jnp.logical_or(mine, is_late) if t == 2 else mine

            @pl.when(jnp.logical_not(skip))
            def _():
                landed(d, main_r.at[(ys * FS + zs) * N_T + t])

    def piece(yy, q, zz, lo=0, hi=hot):
        col = pl.multiple_of(zz * width, width)
        rows = pl.ds(pl.multiple_of(q * cut_g, cut_g), cut_g)
        slots = pl.ds(lo, hi - lo)
        return (
            hot13.at[yy, slots, rows, pl.ds(col, width)],
            hot13.at[yy, slots, rows, pl.ds(pl.multiple_of(full + col, width), width)],
            hot2.at[yy, slots, pl.ds(pl.multiple_of(col + q * cut_d, cut_d), cut_d), :],
        )

    half = hot // 2
    q_x, q_p = 2 * (1 - x) + c, 2 * x + (1 - c)
    to_x, to_y, to_p = (z, p, q_x), (z, 1 - p, e), (z, p, q_p)

    def send(src, dst, ss, rs, i, to):
        for t in range(N_T):
            remote(src[t], dst[t], ss.at[i * N_T + t], rs.at[i * N_T + t], to).start()

    def sent(src, ss, i, to):
        for t in range(N_T):
            remote(src[t], src[t], ss.at[i * N_T + t], ss.at[i * N_T + t], to).wait_send()

    def arrived(dst, rs, i):
        for t in range(N_T):
            landed(dst[t], rs.at[i * N_T + t])

    def part(q):
        return (
            hot_g.at[:, pl.ds(pl.multiple_of(q * cut_g, cut_g), cut_g), :],
            hot_u.at[:, pl.ds(pl.multiple_of(q * cut_g, cut_g), cut_g), :],
            hot_d.at[:, pl.ds(pl.multiple_of(q * cut_d, cut_d), cut_d), :],
        )

    got = (got_g, got_u, got_d)
    got_x = (got_xg, got_xu, got_xd)
    snd = (snd_g, snd_u, snd_d)
    keep = (keep_g, keep_u, keep_d)
    picked = (hot_g, hot_u, hot_d)
    cut = (cut_g, cut_g, cut_d)
    for xx in range(2):
        for t in range(N_T):
            i = xx * N_T + t
            remote(part(2 * xx + 1 - c)[t], got[t].at[xx], rs_s.at[i], rs_r.at[i], to_p).start()
    after_step()
    for xx in range(2):
        for t in range(N_T):
            landed(got[t].at[xx], rs_r.at[xx * N_T + t])

    def of_chip(xx, out):
        for h in range(hot):
            here = lax.rem(ids[h] // exp_per_ep, 2) == c
            for t in range(N_T):
                rows = pl.ds(pl.multiple_of((2 * xx + c) * cut[t], cut[t]), cut[t])
                out[t][h] = jnp.where(here, picked[t][h, rows, :], got[t][xx, h])

    of_chip(1 - x, snd)
    of_chip(x, keep)
    for t in range(N_T):
        i = 2 * N_T + t
        remote(snd[t], got_x[t], rs_s.at[i], rs_r.at[i], to_x).start()
    for t in range(N_T):
        landed(got_x[t], rs_r.at[2 * N_T + t])
    for h in range(hot):
        here = ids[h] // exp_per_ep // 2 == x
        for t in range(N_T):
            (sel_g, sel_u, sel_d)[t][h] = jnp.where(here, keep[t][h], got_x[t][h])
    sel = (sel_g, sel_u, sel_d)

    def broadcast(src, zz, k):
        dst = piece(p, e, zz)
        send(src, dst, x_s, x_r, k, to_x)
        send(src, dst, y_s, y_r, k, to_y)
        send(src, dst, p_s, p_r, k, to_p)

    mine = piece(p, e, z)
    UP, DOWN = 0, 1

    @pl.when(z < FS - 1)
    def _():
        send(sel, mine, z_s, z_r, UP * FS + 1, (z + 1, p, e))

    @pl.when(z > 0)
    def _():
        send(sel, mine, z_s, z_r, DOWN * FS + 1, (z - 1, p, e))

    broadcast(sel, z, z)
    after_step()
    for t in range(N_T):
        pltpu.make_async_copy(sel[t], mine[t], own.at[t]).start()

    def z_step(k):
        @pl.when(z - k >= 0)
        def _():
            src = piece(p, e, z - k)
            arrived(src, z_r, UP * FS + k)

            @pl.when(z < FS - 1)
            def _():
                send(src, src, z_s, z_r, UP * FS + k + 1, (z + 1, p, e))

            broadcast(src, z - k, z - k)

        @pl.when(z + k < FS)
        def _():
            src = piece(p, e, z + k)
            arrived(src, z_r, DOWN * FS + k)

            @pl.when(z > 0)
            def _():
                send(src, src, z_s, z_r, DOWN * FS + k + 1, (z - 1, p, e))

            broadcast(src, z + k, z + k)

    def plane_step(zz):
        from_x = piece(p, q_x, zz)
        arrived(from_x, x_r, zz)
        a = piece(p, q_x, zz, 0, half)
        send(a, a, da_s, da_r, zz, to_y)
        send(from_x, from_x, px_s, px_r, zz, to_p)
        from_y = piece(1 - p, e, zz)
        arrived(from_y, y_r, zz)
        b = piece(1 - p, e, zz, half, hot)
        send(b, b, db_s, db_r, zz, to_x)
        send(from_y, from_y, py_s, py_r, zz, to_p)

    def diagonal_step(zz):
        a = piece(1 - p, q_x, zz, 0, half)
        arrived(a, da_r, zz)
        send(a, a, pa_s, pa_r, zz, to_p)
        b = piece(1 - p, q_x, zz, half, hot)
        arrived(b, db_r, zz)
        send(b, b, pb_s, pb_r, zz, to_p)

    for k in range(1, FS):
        z_step(k)
        after_step()
    for k in range(FS):
        plane_step(lax.rem(z + k, FS))
        after_step()
    for k in range(FS):
        diagonal_step(lax.rem(z + k, FS))
        after_step()
    after_step()

    for t in range(N_T):
        pltpu.make_async_copy(sel[t], mine[t], own.at[t]).wait()
    for i in range(3 * N_T):
        t = i % N_T
        remote(sel[t], sel[t], rs_s.at[i], rs_s.at[i], to_p).wait_send()
    for k in range(1, FS):
        @pl.when(jnp.logical_and(z - k + 1 >= 0, z < FS - 1))
        def _():
            sent(mine, z_s, UP * FS + k, (z + 1, p, e))

        @pl.when(jnp.logical_and(z + k - 1 < FS, z > 0))
        def _():
            sent(mine, z_s, DOWN * FS + k, (z - 1, p, e))
    for zz in range(FS):
        src = piece(p, e, zz)
        sent(src, x_s, zz, to_x)
        sent(src, y_s, zz, to_y)
        sent(src, p_s, zz, to_p)
        sent(src, px_s, zz, to_p)
        sent(src, py_s, zz, to_p)
        a = piece(p, q_x, zz, 0, half)
        b = piece(p, q_x, zz, half, hot)
        sent(a, da_s, zz, to_y)
        sent(b, db_s, zz, to_x)
        sent(a, pa_s, zz, to_p)
        sent(b, pb_s, zz, to_p)
        q_px = 2 * (1 - x) + (1 - c)
        arrived(piece(p, q_p, zz), p_r, zz)
        arrived(piece(p, q_px, zz), px_r, zz)
        arrived(piece(1 - p, q_p, zz), py_r, zz)
        arrived(piece(1 - p, q_px, zz, 0, half), pa_r, zz)
        arrived(piece(1 - p, q_px, zz, half, hot), pb_r, zz)
    for t in range(N_T):
        for kk in range(FS):
            zz = lax.rem(z + kk, FS)
            if (kk, t) == (LATE, 2):
                main_sent(zz, 1 - p, t)
            else:
                main_sent(zz, 0, t)
                main_sent(zz, 1, t)
    pltpu.make_async_copy(late_src, late, loc.at[N_T]).wait()
    for ys in range(PP):
        for zs in range(FS):
            main_landed(ys, zs)


def exchange(ids, w_gate, w_up, w_down, hot_g, hot_u, hot_d):
    dt = w_gate.dtype
    exp_local, d, f = w_gate.shape[1:]
    hot = hot_g.shape[0]
    per_dev = exp_local // (FS * PP)
    full = f * FS
    dma = lambda n: pltpu.SemaphoreType.DMA((n,))
    quarter = [(hot, d // EP, f), (hot, d // EP, f), (hot, f // EP, d)]
    four = lambda: [dma(FS * N_T), dma(FS * N_T)]
    return pl.pallas_call(
        functools.partial(exchange_body, exp_local),
        out_shape=(
            pltpu.HBM((PP, per_dev, d, 2 * full), dt),
            pltpu.HBM((PP, per_dev, full, d), dt),
            pltpu.HBM((PP, hot, d, 2 * full), dt),
            pltpu.HBM((PP, hot, full, d), dt),
            pltpu.HBM((per_dev, f, d), dt),
        ),
        in_specs=[pl.BlockSpec(memory_space=pltpu.SMEM)] + [HBM] * N_T + [VMEM] * N_T,
        out_specs=(HBM,) * 5,
        scratch_shapes=[pltpu.VMEM((2,) + s, dt) for s in quarter]
        + [pltpu.VMEM(s, dt) for s in quarter] * 4
        + [dma(FS * PP * N_T), dma(FS * PP * N_T), dma(EP * N_T), dma(EP * N_T), dma(N_T + 1), dma(N_T)]
        + [dma(2 * FS * N_T), dma(2 * FS * N_T)]
        + four() * 9,
        compiler_params=pltpu.CompilerParams(has_side_effects=True, vmem_limit_bytes=16 << 20),
        name="exchange",
    )(ids, w_gate, w_up, w_down, hot_g, hot_u, hot_d)


def settle_body(n_slot, ahead, *refs):
    n = (len(refs) - 3) // 2
    src, dst, (buf, r_sem, w_sem) = refs[:n], refs[n : 2 * n], refs[2 * n :]
    steps = [(a, i, j) for a in range(n) for i in range(src[a].shape[0]) for j in range(src[a].shape[1])]

    def load(k):
        a, i, j = steps[k]
        return pltpu.make_async_copy(src[a].at[i, j], buf.at[k % n_slot, pl.ds(0, src[a].shape[2])], r_sem.at[k % n_slot])

    def store(k):
        a, i, j = steps[k]
        return pltpu.make_async_copy(buf.at[k % n_slot, pl.ds(0, src[a].shape[2])], dst[a].at[i, j], w_sem.at[k % n_slot])

    for k in range(min(ahead, len(steps))):
        load(k).start()
    for k in range(len(steps)):
        load(k).wait()
        store(k).start()
        if k + ahead < len(steps):
            if k + ahead >= n_slot:
                store(k + ahead - n_slot).wait()
            load(k + ahead).start()
    for k in range(max(0, len(steps) - n_slot), len(steps)):
        store(k).wait()


def settle(*arrays):
    n_slot, ahead = 12, 6
    rows = max(a.shape[2] for a in arrays)
    size = sum(a.size * a.dtype.itemsize for a in arrays)
    return pl.pallas_call(
        functools.partial(settle_body, n_slot, ahead),
        out_shape=tuple(jax.ShapeDtypeStruct(a.shape, a.dtype) for a in arrays),
        in_specs=[HBM] * len(arrays),
        out_specs=(HBM,) * len(arrays),
        scratch_shapes=[
            pltpu.VMEM((n_slot, rows, arrays[0].shape[3]), arrays[0].dtype),
            pltpu.SemaphoreType.DMA((n_slot,)),
            pltpu.SemaphoreType.DMA((n_slot,)),
        ],
        cost_estimate=pl.CostEstimate(flops=size * 16, bytes_accessed=2 * size, transcendentals=0),
        name="settle",
    )(*arrays)


def insert_body(piece, whole_in, whole_out, sem):
    f = piece.shape[1]
    lay, zz = lax.rem(lax.axis_index("ep"), 2), lax.rem(lax.axis_index("fs") + LATE, FS)
    at = whole_out.at[lay, :, pl.ds(pl.multiple_of(zz * f, f), f), :]
    copy = pltpu.make_async_copy(piece, at, sem)
    copy.start()
    copy.wait()


def insert(whole, piece):
    return pl.pallas_call(
        insert_body,
        out_shape=jax.ShapeDtypeStruct(whole.shape, whole.dtype),
        in_specs=[pl.BlockSpec(memory_space=pltpu.VMEM), HBM],
        out_specs=HBM,
        scratch_shapes=[pltpu.SemaphoreType.DMA],
        compiler_params=pltpu.CompilerParams(vmem_limit_bytes=4 << 20),
        input_output_aliases={1: 0},
        name="insert",
    )(piece, whole)


def late_pairs():
    flat = lambda z, p, e: (z * PP + p) * EP + e
    return [
        (flat(z, p, e), flat((z + LATE) % FS, e // 2, (2 * e + p) % EP))
        for z in range(FS)
        for p in range(PP)
        for e in range(EP)
    ]


def solution(mesh):
    in_spec = P("pp", "ep", None, "fs")
    down_spec = P("pp", "ep", "fs", None)
    home_spec = P(None, ("pp", "ep", "fs"), None, None)

    def device_body(w_gate, w_up, w_down, hot_ids):
        w_gate, w_up, w_down = in_hbm(w_gate), in_hbm(w_up), in_hbm(w_down)
        picked = map(in_vmem, pick(hot_ids, w_gate, w_up, w_down))
        *came, late = exchange(hot_ids, w_gate, w_up, w_down, *picked)
        late = lax.ppermute(late, ("fs", "pp", "ep"), late_pairs())
        w13, w2, hot13, hot2 = settle(*came)
        w2 = insert(w2, late)
        return w13, w2, hot13, hot2

    return jax.shard_map(
        device_body,
        mesh=mesh,
        in_specs=(in_spec, in_spec, down_spec, P()),
        out_specs=(home_spec, home_spec, P(), P()),
        check_vma=False,
    )
```

```python
import functools

import jax
import jax.numpy as jnp
from jax import lax
from jax.experimental import pallas as pl
from jax.experimental.pallas import tpu as pltpu
from jax.sharding import PartitionSpec as P

ANY = pl.BlockSpec(memory_space=pl.ANY)
HBM = pl.BlockSpec(memory_space=pltpu.HBM)
VMEM = pl.BlockSpec(memory_space=pltpu.VMEM)
MESH = pl.DeviceIdType.MESH
FS, PP, EP = 4, 2, 4
N_T = 3
LATE = 2
OUTER = [(m, b, t) for t in range(N_T) for b in range(2) for m in (1, 3, 2, 0) if (m, t) != (2, 2)]
INNER = [(m, b, t) for t in range(N_T) for b in range(2) for m in (2, 0, 3, 1) if (m, t) != (3, 2)]
COUNTS = (4, 0, 0, 0, 24)


def in_hbm(a):
    return pltpu.with_memory_space_constraint(a, pltpu.HBM)


def in_vmem(a):
    return pltpu.with_memory_space_constraint(a, pltpu.VMEM)


def pick_body(exp_per_ep, ids, gate, up, down, gate_out, up_out, down_out, sems):
    base = lax.axis_index("ep") * exp_per_ep
    copies = []
    for h in range(gate_out.shape[0]):
        held = jnp.clip(ids[h] - base, 0, exp_per_ep - 1)
        for t, (s, d) in enumerate(((gate, gate_out), (up, up_out), (down, down_out))):
            copies.append(pltpu.make_async_copy(s.at[0, held], d.at[h], sems.at[h * N_T + t]))
    for copy in copies:
        copy.start()
    for copy in copies:
        copy.wait()


def pick(ids, w_gate, w_up, w_down):
    hot = ids.shape[0]
    exp_local, d, f = w_gate.shape[1:]
    dt = w_gate.dtype
    return pl.pallas_call(
        functools.partial(pick_body, exp_local),
        out_shape=(pltpu.VMEM((hot, d, f), dt), pltpu.VMEM((hot, d, f), dt), pltpu.VMEM((hot, f, d), dt)),
        in_specs=[pl.BlockSpec(memory_space=pltpu.SMEM)] + [HBM] * N_T,
        out_specs=(pl.BlockSpec(memory_space=pltpu.VMEM),) * N_T,
        scratch_shapes=[pltpu.SemaphoreType.DMA((hot * N_T,))],
        compiler_params=pltpu.CompilerParams(vmem_limit_bytes=4 << 20),
        name="pick",
    )(ids, w_gate, w_up, w_down)


def exchange_body(
    exp_per_ep, ids, gate, up, down, hot_g, hot_u, hot_d, w13, w2, hot13, hot2, late,
    got_g, got_u, got_d, got_xg, got_xu, got_xd, snd_g, snd_u, snd_d, keep_g, keep_u, keep_d, sel_g, sel_u, sel_d,
    main_s, main_r, rs_s, rs_r, loc, own, z_s, z_r, x_s, x_r, y_s, y_r, p_s, p_r, da_s, da_r, db_s, db_r, px_s, px_r, py_s, py_r, pa_s, pa_r, pb_s, pb_r,
):
    z, p, e = lax.axis_index("fs"), lax.axis_index("pp"), lax.axis_index("ep")
    x, c = e // 2, lax.rem(e, 2)
    width = gate.shape[3]
    hot = hot_g.shape[0]
    cut_g, cut_d = hot_g.shape[1] // EP, hot_d.shape[1] // EP
    full = gate.shape[3] * FS

    def remote(s, d, ss, rs, to):
        return pltpu.make_async_remote_copy(s, d, ss, rs, device_id=to, device_id_type=MESH)

    def landed(d, rs):
        pltpu.make_async_copy(d, d, rs).wait()

    def home(lay, zz):
        col = pl.multiple_of(zz * width, width)
        return (
            w13.at[lay, :, :, pl.ds(col, width)],
            w13.at[lay, :, :, pl.ds(pl.multiple_of(full + col, width), width)],
            w2.at[lay, :, pl.ds(col, width), :],
        )

    def main_to(zz, b):
        return (zz, x, lax.rem(2 * e + b, EP))

    def main_is_self(zz, b):
        return jnp.logical_and(jnp.logical_and(x == p, lax.rem(2 * e + b, EP) == e), zz == z)

    def main_copy(zz, b, t):
        k = b * FS + zz
        return (gate, up, down)[t].at[0, pl.ds(3 * k, 3)], home(p, z)[t], k * N_T + t

    def main_start(zz, b, t):
        mine = main_is_self(zz, b)
        s, d, i = main_copy(zz, b, t)

        @pl.when(jnp.logical_not(mine))
        def _():
            remote(s, d, main_s.at[i], main_r.at[(p * FS + z) * N_T + t], main_to(zz, b)).start()

        @pl.when(mine)
        def _():
            pltpu.make_async_copy(s, d, loc.at[t]).start()

    def main_sent(zz, b, t):
        mine = main_is_self(zz, b)
        s, d, i = main_copy(zz, b, t)

        @pl.when(jnp.logical_not(mine))
        def _():
            remote(s, d, main_s.at[i], main_s.at[i], main_to(zz, b)).wait_send()

        @pl.when(mine)
        def _():
            pltpu.make_async_copy(s, d, loc.at[t]).wait()

    upper = z // 2
    inner = z * (1 - upper) + (FS - 1 - z) * upper

    def group(items):
        for m, b, t in items:
            main_start(m * (1 - upper) + (FS - 1 - m) * upper, b, t)

    bounds = [0]

    def after_step():
        lo = bounds[-1]
        step = len(bounds) - 1
        hi = min(len(OUTER), lo + (COUNTS[step] if step < len(COUNTS) else len(OUTER)))
        bounds.append(hi)
        if hi > lo:
            pl.when(inner == 0)(lambda: group(OUTER[lo:hi]))
            pl.when(inner == 1)(lambda: group(INNER[lo:hi]))

    late_src = down.at[0, pl.ds(3 * (p * FS + lax.rem(z + LATE, FS)), 3)]
    pltpu.make_async_copy(late_src, late, loc.at[N_T]).start()
    def main_landed(ys, zs):
        mine = jnp.logical_and(jnp.logical_and(2 * p + x == e, p == ys), z == zs)

        outside = zs == lax.rem(z + LATE, FS)
        for t, d in enumerate(home(ys, zs)):
            skip = jnp.logical_or(mine, outside) if t == 2 else mine

            @pl.when(jnp.logical_not(skip))
            def _():
                landed(d, main_r.at[(ys * FS + zs) * N_T + t])

    def piece(yy, q, zz, lo=0, hi=hot):
        col = pl.multiple_of(zz * width, width)
        rows = pl.ds(pl.multiple_of(q * cut_g, cut_g), cut_g)
        slots = pl.ds(lo, hi - lo)
        return (
            hot13.at[yy, slots, rows, pl.ds(col, width)],
            hot13.at[yy, slots, rows, pl.ds(pl.multiple_of(full + col, width), width)],
            hot2.at[yy, slots, pl.ds(pl.multiple_of(col + q * cut_d, cut_d), cut_d), :],
        )

    half = hot // 2
    q_x, q_p = 2 * (1 - x) + c, 2 * x + (1 - c)
    to_x, to_y, to_p = (z, p, q_x), (z, 1 - p, e), (z, p, q_p)

    def send(src, dst, ss, rs, i, to):
        for t in range(N_T):
            remote(src[t], dst[t], ss.at[i * N_T + t], rs.at[i * N_T + t], to).start()

    def sent(src, ss, i, to):
        for t in range(N_T):
            remote(src[t], src[t], ss.at[i * N_T + t], ss.at[i * N_T + t], to).wait_send()

    def arrived(dst, rs, i):
        for t in range(N_T):
            landed(dst[t], rs.at[i * N_T + t])

    def part(q):
        return (
            hot_g.at[:, pl.ds(pl.multiple_of(q * cut_g, cut_g), cut_g), :],
            hot_u.at[:, pl.ds(pl.multiple_of(q * cut_g, cut_g), cut_g), :],
            hot_d.at[:, pl.ds(pl.multiple_of(q * cut_d, cut_d), cut_d), :],
        )

    got = (got_g, got_u, got_d)
    got_x = (got_xg, got_xu, got_xd)
    snd = (snd_g, snd_u, snd_d)
    keep = (keep_g, keep_u, keep_d)
    picked = (hot_g, hot_u, hot_d)
    cut = (cut_g, cut_g, cut_d)
    for xx in range(2):
        for t in range(N_T):
            i = xx * N_T + t
            remote(part(2 * xx + 1 - c)[t], got[t].at[xx], rs_s.at[i], rs_r.at[i], to_p).start()
    after_step()
    for xx in range(2):
        for t in range(N_T):
            landed(got[t].at[xx], rs_r.at[xx * N_T + t])

    def of_chip(xx, out):
        for h in range(hot):
            here = lax.rem(ids[h] // exp_per_ep, 2) == c
            for t in range(N_T):
                rows = pl.ds(pl.multiple_of((2 * xx + c) * cut[t], cut[t]), cut[t])
                out[t][h] = jnp.where(here, picked[t][h, rows, :], got[t][xx, h])

    of_chip(1 - x, snd)
    of_chip(x, keep)
    for t in range(N_T):
        i = 2 * N_T + t
        remote(snd[t], got_x[t], rs_s.at[i], rs_r.at[i], to_x).start()
    for t in range(N_T):
        landed(got_x[t], rs_r.at[2 * N_T + t])
    for h in range(hot):
        here = ids[h] // exp_per_ep // 2 == x
        for t in range(N_T):
            (sel_g, sel_u, sel_d)[t][h] = jnp.where(here, keep[t][h], got_x[t][h])
    sel = (sel_g, sel_u, sel_d)

    def broadcast(src, zz, k):
        dst = piece(p, e, zz)
        send(src, dst, x_s, x_r, k, to_x)
        send(src, dst, y_s, y_r, k, to_y)
        send(src, dst, p_s, p_r, k, to_p)

    mine = piece(p, e, z)
    UP, DOWN = 0, 1

    @pl.when(z < FS - 1)
    def _():
        send(sel, mine, z_s, z_r, UP * FS + 1, (z + 1, p, e))

    @pl.when(z > 0)
    def _():
        send(sel, mine, z_s, z_r, DOWN * FS + 1, (z - 1, p, e))

    broadcast(sel, z, z)
    after_step()
    for t in range(N_T):
        pltpu.make_async_copy(sel[t], mine[t], own.at[t]).start()

    def z_step(k):
        @pl.when(z - k >= 0)
        def _():
            src = piece(p, e, z - k)
            arrived(src, z_r, UP * FS + k)

            @pl.when(z < FS - 1)
            def _():
                send(src, src, z_s, z_r, UP * FS + k + 1, (z + 1, p, e))

            broadcast(src, z - k, z - k)

        @pl.when(z + k < FS)
        def _():
            src = piece(p, e, z + k)
            arrived(src, z_r, DOWN * FS + k)

            @pl.when(z > 0)
            def _():
                send(src, src, z_s, z_r, DOWN * FS + k + 1, (z - 1, p, e))

            broadcast(src, z + k, z + k)

    def plane_step(zz):
        from_x = piece(p, q_x, zz)
        arrived(from_x, x_r, zz)
        a = piece(p, q_x, zz, 0, half)
        send(a, a, da_s, da_r, zz, to_y)
        send(from_x, from_x, px_s, px_r, zz, to_p)
        from_y = piece(1 - p, e, zz)
        arrived(from_y, y_r, zz)
        b = piece(1 - p, e, zz, half, hot)
        send(b, b, db_s, db_r, zz, to_x)
        send(from_y, from_y, py_s, py_r, zz, to_p)

    def diagonal_step(zz):
        a = piece(1 - p, q_x, zz, 0, half)
        arrived(a, da_r, zz)
        send(a, a, pa_s, pa_r, zz, to_p)
        b = piece(1 - p, q_x, zz, half, hot)
        arrived(b, db_r, zz)
        send(b, b, pb_s, pb_r, zz, to_p)

    for k in range(1, FS):
        z_step(k)
        after_step()
    for k in range(FS):
        plane_step(lax.rem(z + k, FS))
        after_step()
    for k in range(FS):
        diagonal_step(lax.rem(z + k, FS))
        after_step()
    after_step()

    for t in range(N_T):
        pltpu.make_async_copy(sel[t], mine[t], own.at[t]).wait()
    for i in range(3 * N_T):
        t = i % N_T
        remote(sel[t], sel[t], rs_s.at[i], rs_s.at[i], to_p).wait_send()
    for k in range(1, FS):
        @pl.when(jnp.logical_and(z - k + 1 >= 0, z < FS - 1))
        def _():
            sent(mine, z_s, UP * FS + k, (z + 1, p, e))

        @pl.when(jnp.logical_and(z + k - 1 < FS, z > 0))
        def _():
            sent(mine, z_s, DOWN * FS + k, (z - 1, p, e))
    for zz in range(FS):
        src = piece(p, e, zz)
        sent(src, x_s, zz, to_x)
        sent(src, y_s, zz, to_y)
        sent(src, p_s, zz, to_p)
        sent(src, px_s, zz, to_p)
        sent(src, py_s, zz, to_p)
        a = piece(p, q_x, zz, 0, half)
        b = piece(p, q_x, zz, half, hot)
        sent(a, da_s, zz, to_y)
        sent(b, db_s, zz, to_x)
        sent(a, pa_s, zz, to_p)
        sent(b, pb_s, zz, to_p)
        q_px = 2 * (1 - x) + (1 - c)
        arrived(piece(p, q_p, zz), p_r, zz)
        arrived(piece(p, q_px, zz), px_r, zz)
        arrived(piece(1 - p, q_p, zz), py_r, zz)
        arrived(piece(1 - p, q_px, zz, 0, half), pa_r, zz)
        arrived(piece(1 - p, q_px, zz, half, hot), pb_r, zz)
    for t in range(N_T):
        for kk in range(FS):
            zz = lax.rem(z + kk, FS)
            if (kk, t) != (LATE, 2):
                main_sent(zz, 0, t)
                main_sent(zz, 1, t)
    pltpu.make_async_copy(late_src, late, loc.at[N_T]).wait()
    for ys in range(PP):
        for zs in range(FS):
            main_landed(ys, zs)


def exchange(ids, w_gate, w_up, w_down, hot_g, hot_u, hot_d):
    dt = w_gate.dtype
    exp_local, d, f = w_gate.shape[1:]
    hot = hot_g.shape[0]
    per_dev = exp_local // (FS * PP)
    full = f * FS
    dma = lambda n: pltpu.SemaphoreType.DMA((n,))
    quarter = [(hot, d // EP, f), (hot, d // EP, f), (hot, f // EP, d)]
    four = lambda: [dma(FS * N_T), dma(FS * N_T)]
    return pl.pallas_call(
        functools.partial(exchange_body, exp_local),
        out_shape=(
            pltpu.HBM((PP, per_dev, d, 2 * full), dt),
            pltpu.HBM((PP, per_dev, full, d), dt),
            pltpu.HBM((PP, hot, d, 2 * full), dt),
            pltpu.VMEM((PP, hot, full, d), dt),
            pltpu.HBM((per_dev, f, d), dt),
        ),
        in_specs=[pl.BlockSpec(memory_space=pltpu.SMEM)] + [HBM] * N_T + [VMEM] * N_T,
        out_specs=(HBM, HBM, HBM, VMEM, HBM),
        scratch_shapes=[pltpu.VMEM((2,) + s, dt) for s in quarter]
        + [pltpu.VMEM(s, dt) for s in quarter] * 4
        + [dma(FS * PP * N_T), dma(FS * PP * N_T), dma(EP * N_T), dma(EP * N_T), dma(N_T + 1), dma(N_T)]
        + [dma(2 * FS * N_T), dma(2 * FS * N_T)]
        + four() * 9,
        compiler_params=pltpu.CompilerParams(has_side_effects=True, vmem_limit_bytes=16 << 20),
        cost_estimate=pl.CostEstimate(flops=1 << 36, bytes_accessed=1 << 27, transcendentals=0),
        name="exchange",
    )(ids, w_gate, w_up, w_down, hot_g, hot_u, hot_d)


def place_of(piece, whole, lay):
    f = piece.shape[1]
    zz = lax.rem(lax.axis_index("fs") + LATE, FS)
    return whole.at[lay, :, pl.ds(pl.multiple_of(zz * f, f), f), :]


def settle_body(n_slot, ahead, w13, w2, hot13, hot2, early, w13_out, w2_out, hot13_out, hot2_out, buf, r_sem, w_sem, hot_sem, early_sem):
    steps = [
        (src, dst, i, j)
        for src, dst in ((w2, w2_out), (w13, w13_out), (hot13, hot13_out))
        for i in range(src.shape[0])
        for j in range(src.shape[1])
    ]
    n_first = w2.shape[0] * w2.shape[1]
    direct = [pltpu.make_async_copy(hot2.at[i], hot2_out.at[i], hot_sem.at[i]) for i in range(hot2.shape[0])]
    core = lax.rem(lax.axis_index("ep"), 2)
    early_copy = pltpu.make_async_copy(early, place_of(early, w2_out, 1 - core), early_sem)

    def load(k):
        src, dst, i, j = steps[k]
        return pltpu.make_async_copy(src.at[i, j], buf.at[k % n_slot, pl.ds(0, src.shape[2])], r_sem.at[k % n_slot])

    def store(k):
        src, dst, i, j = steps[k]
        return pltpu.make_async_copy(buf.at[k % n_slot, pl.ds(0, src.shape[2])], dst.at[i, j], w_sem.at[k % n_slot])

    for k in range(ahead):
        load(k).start()
    for copy in direct:
        copy.start()
    for k in range(len(steps)):
        load(k).wait()
        store(k).start()
        if k + ahead < len(steps):
            old = k + ahead - n_slot
            if old >= 0:
                store(old).wait()
            if old == n_first - 1:
                early_copy.start()
            load(k + ahead).start()
    for k in range(len(steps) - n_slot, len(steps)):
        store(k).wait()
    for copy in direct:
        copy.wait()
    early_copy.wait()


def settle(w13, w2, hot13, hot2, early):
    n_slot, ahead = 12, 7
    arrays = [in_hbm(w13), in_hbm(w2), in_hbm(hot13), in_vmem(hot2)]
    size = sum(a.size * a.dtype.itemsize for a in arrays)
    return pl.pallas_call(
        functools.partial(settle_body, n_slot, ahead),
        out_shape=tuple(pltpu.HBM(a.shape, a.dtype) for a in arrays),
        in_specs=[HBM, HBM, HBM, VMEM, VMEM],
        out_specs=(HBM,) * len(arrays),
        scratch_shapes=[
            pltpu.VMEM((n_slot,) + w13.shape[2:], w13.dtype),
            pltpu.SemaphoreType.DMA((n_slot,)),
            pltpu.SemaphoreType.DMA((n_slot,)),
            pltpu.SemaphoreType.DMA((PP,)),
            pltpu.SemaphoreType.DMA,
        ],
        compiler_params=pltpu.CompilerParams(vmem_limit_bytes=26 << 20),
        cost_estimate=pl.CostEstimate(flops=size * 16, bytes_accessed=2 * size, transcendentals=0),
        name="settle",
    )(*arrays, early)


def insert_body(piece, whole_in, whole_out, sem):
    copy = pltpu.make_async_copy(piece, place_of(piece, whole_out, lax.rem(lax.axis_index("ep"), 2)), sem)
    copy.start()
    copy.wait()


def insert(whole, piece):
    return pl.pallas_call(
        insert_body,
        out_shape=jax.ShapeDtypeStruct(whole.shape, whole.dtype),
        in_specs=[pl.BlockSpec(memory_space=pltpu.VMEM), HBM],
        out_specs=HBM,
        scratch_shapes=[pltpu.SemaphoreType.DMA],
        compiler_params=pltpu.CompilerParams(vmem_limit_bytes=4 << 20),
        input_output_aliases={1: 0},
        name="insert",
    )(piece, whole)


def stage_body(down, out, sem):
    z, p = lax.axis_index("fs"), lax.axis_index("pp")
    n = out.shape[0]
    copy = pltpu.make_async_copy(down.at[0, pl.ds(n * ((1 - p) * FS + lax.rem(z + LATE, FS)), n)], out, sem)
    copy.start()
    copy.wait()


def stage(w_down):
    exp_local, f, d = w_down.shape[1:]
    return pl.pallas_call(
        stage_body,
        out_shape=pltpu.VMEM((exp_local // (FS * PP), f, d), w_down.dtype),
        in_specs=[HBM],
        out_specs=VMEM,
        scratch_shapes=[pltpu.SemaphoreType.DMA],
        compiler_params=pltpu.CompilerParams(vmem_limit_bytes=4 << 20),
        name="stage",
    )(w_down)


def piece_pairs(core_of_stage):
    flat = lambda z, p, e: (z * PP + p) * EP + e
    return [
        (flat(z, p, e), flat((z + LATE) % FS, e // 2, (2 * e + core_of_stage(p)) % EP))
        for z in range(FS)
        for p in range(PP)
        for e in range(EP)
    ]


def solution(mesh):
    in_spec = P("pp", "ep", None, "fs")
    down_spec = P("pp", "ep", "fs", None)
    home_spec = P(None, ("pp", "ep", "fs"), None, None)

    def device_body(w_gate, w_up, w_down, hot_ids):
        w_gate, w_up, w_down = in_hbm(w_gate), in_hbm(w_up), in_hbm(w_down)
        early = lax.ppermute(stage(w_down), ("fs", "pp", "ep"), piece_pairs(lambda p: 1 - p))
        picked = map(in_vmem, pick(hot_ids, w_gate, w_up, w_down))
        *came, late = exchange(hot_ids, w_gate, w_up, w_down, *picked)
        late = lax.ppermute(late, ("fs", "pp", "ep"), piece_pairs(lambda p: p))
        w13, w2, hot13, hot2 = settle(*came, early)
        w2 = insert(w2, late)
        return w13, w2, hot13, hot2

    return jax.shard_map(
        device_body,
        mesh=mesh,
        in_specs=(in_spec, in_spec, down_spec, P()),
        out_specs=(home_spec, home_spec, P(), P()),
        check_vma=False,
    )
```

```python
import functools

import jax
import jax.numpy as jnp
from jax import lax
from jax.experimental import pallas as pl
from jax.experimental.pallas import tpu as pltpu
from jax.sharding import PartitionSpec as P

ANY = pl.BlockSpec(memory_space=pl.ANY)
HBM = pl.BlockSpec(memory_space=pltpu.HBM)
VMEM = pl.BlockSpec(memory_space=pltpu.VMEM)
MESH = pl.DeviceIdType.MESH
FS, PP, EP = 4, 2, 4
N_T = 3
LATE = 2
OUTER = [(m, b, t) for t in range(N_T) for b in range(2) for m in (1, 3, 2, 0) if (m, t) != (2, 2)]
INNER = [(m, b, t) for t in range(N_T) for b in range(2) for m in (2, 0, 3, 1) if (m, t) != (3, 2)]
COUNTS = (2, 0, 2, 0, 24)


def in_hbm(a):
    return pltpu.with_memory_space_constraint(a, pltpu.HBM)


def in_vmem(a):
    return pltpu.with_memory_space_constraint(a, pltpu.VMEM)


def pick_body(exp_per_ep, ids, gate, up, down, gate_out, up_out, down_out, sems):
    base = lax.axis_index("ep") * exp_per_ep
    copies = []
    for h in range(gate_out.shape[0]):
        held = jnp.clip(ids[h] - base, 0, exp_per_ep - 1)
        for t, (s, d) in enumerate(((gate, gate_out), (up, up_out), (down, down_out))):
            copies.append(pltpu.make_async_copy(s.at[0, held], d.at[h], sems.at[h * N_T + t]))
    for copy in copies:
        copy.start()
    for copy in copies:
        copy.wait()


def pick(ids, w_gate, w_up, w_down):
    hot = ids.shape[0]
    exp_local, d, f = w_gate.shape[1:]
    dt = w_gate.dtype
    return pl.pallas_call(
        functools.partial(pick_body, exp_local),
        out_shape=(pltpu.VMEM((hot, d, f), dt), pltpu.VMEM((hot, d, f), dt), pltpu.VMEM((hot, f, d), dt)),
        in_specs=[pl.BlockSpec(memory_space=pltpu.SMEM)] + [HBM] * N_T,
        out_specs=(pl.BlockSpec(memory_space=pltpu.VMEM),) * N_T,
        scratch_shapes=[pltpu.SemaphoreType.DMA((hot * N_T,))],
        compiler_params=pltpu.CompilerParams(vmem_limit_bytes=4 << 20),
        name="pick",
    )(ids, w_gate, w_up, w_down)


def exchange_body(
    exp_per_ep, ids, gate, up, down, hot_g, hot_u, hot_d, w13, w2, hot13, hot2, late,
    got_g, got_u, got_d, got_xg, got_xu, got_xd, snd_g, snd_u, snd_d, keep_g, keep_u, keep_d, sel_g, sel_u, sel_d,
    main_s, main_r, rs_s, rs_r, loc, own, z_s, z_r, x_s, x_r, y_s, y_r, p_s, p_r, da_s, da_r, db_s, db_r, px_s, px_r, py_s, py_r, pa_s, pa_r, pb_s, pb_r,
):
    z, p, e = lax.axis_index("fs"), lax.axis_index("pp"), lax.axis_index("ep")
    x, c = e // 2, lax.rem(e, 2)
    width = gate.shape[3]
    hot = hot_g.shape[0]
    cut_g, cut_d = hot_g.shape[1] // EP, hot_d.shape[1] // EP
    full = gate.shape[3] * FS

    def remote(s, d, ss, rs, to):
        return pltpu.make_async_remote_copy(s, d, ss, rs, device_id=to, device_id_type=MESH)

    def landed(d, rs):
        pltpu.make_async_copy(d, d, rs).wait()

    def home(lay, zz):
        col = pl.multiple_of(zz * width, width)
        return (
            w13.at[lay, :, :, pl.ds(col, width)],
            w13.at[lay, :, :, pl.ds(pl.multiple_of(full + col, width), width)],
            w2.at[lay, :, pl.ds(col, width), :],
        )

    def main_to(zz, b):
        return (zz, x, lax.rem(2 * e + b, EP))

    def main_is_self(zz, b):
        return jnp.logical_and(jnp.logical_and(x == p, lax.rem(2 * e + b, EP) == e), zz == z)

    def main_copy(zz, b, t):
        k = b * FS + zz
        return (gate, up, down)[t].at[0, pl.ds(3 * k, 3)], home(p, z)[t], k * N_T + t

    def main_start(zz, b, t):
        mine = main_is_self(zz, b)
        s, d, i = main_copy(zz, b, t)

        @pl.when(jnp.logical_not(mine))
        def _():
            remote(s, d, main_s.at[i], main_r.at[(p * FS + z) * N_T + t], main_to(zz, b)).start()

        @pl.when(mine)
        def _():
            pltpu.make_async_copy(s, d, loc.at[t]).start()

    def main_sent(zz, b, t):
        mine = main_is_self(zz, b)
        s, d, i = main_copy(zz, b, t)

        @pl.when(jnp.logical_not(mine))
        def _():
            remote(s, d, main_s.at[i], main_s.at[i], main_to(zz, b)).wait_send()

        @pl.when(mine)
        def _():
            pltpu.make_async_copy(s, d, loc.at[t]).wait()

    upper = z // 2
    inner = z * (1 - upper) + (FS - 1 - z) * upper

    def group(items):
        for m, b, t in items:
            main_start(m * (1 - upper) + (FS - 1 - m) * upper, b, t)

    bounds = [0]

    def after_step():
        lo = bounds[-1]
        step = len(bounds) - 1
        hi = min(len(OUTER), lo + (COUNTS[step] if step < len(COUNTS) else len(OUTER)))
        bounds.append(hi)
        if hi > lo:
            pl.when(inner == 0)(lambda: group(OUTER[lo:hi]))
            pl.when(inner == 1)(lambda: group(INNER[lo:hi]))

    late_src = down.at[0, pl.ds(3 * (p * FS + lax.rem(z + LATE, FS)), 3)]
    pltpu.make_async_copy(late_src, late, loc.at[N_T]).start()
    def main_landed(ys, zs):
        mine = jnp.logical_and(jnp.logical_and(2 * p + x == e, p == ys), z == zs)

        outside = zs == lax.rem(z + LATE, FS)
        for t, d in enumerate(home(ys, zs)):
            skip = jnp.logical_or(mine, outside) if t == 2 else mine

            @pl.when(jnp.logical_not(skip))
            def _():
                landed(d, main_r.at[(ys * FS + zs) * N_T + t])

    def piece(yy, q, zz, lo=0, hi=hot):
        col = pl.multiple_of(zz * width, width)
        rows = pl.ds(pl.multiple_of(q * cut_g, cut_g), cut_g)
        slots = pl.ds(lo, hi - lo)
        return (
            hot13.at[yy, slots, rows, pl.ds(col, width)],
            hot13.at[yy, slots, rows, pl.ds(pl.multiple_of(full + col, width), width)],
            hot2.at[yy, slots, pl.ds(pl.multiple_of(col + q * cut_d, cut_d), cut_d), :],
        )

    half = hot // 2
    q_x, q_p = 2 * (1 - x) + c, 2 * x + (1 - c)
    to_x, to_y, to_p = (z, p, q_x), (z, 1 - p, e), (z, p, q_p)

    def send(src, dst, ss, rs, i, to):
        for t in range(N_T):
            remote(src[t], dst[t], ss.at[i * N_T + t], rs.at[i * N_T + t], to).start()

    def sent(src, ss, i, to):
        for t in range(N_T):
            remote(src[t], src[t], ss.at[i * N_T + t], ss.at[i * N_T + t], to).wait_send()

    def arrived(dst, rs, i):
        for t in range(N_T):
            landed(dst[t], rs.at[i * N_T + t])

    def part(q):
        return (
            hot_g.at[:, pl.ds(pl.multiple_of(q * cut_g, cut_g), cut_g), :],
            hot_u.at[:, pl.ds(pl.multiple_of(q * cut_g, cut_g), cut_g), :],
            hot_d.at[:, pl.ds(pl.multiple_of(q * cut_d, cut_d), cut_d), :],
        )

    got = (got_g, got_u, got_d)
    got_x = (got_xg, got_xu, got_xd)
    snd = (snd_g, snd_u, snd_d)
    keep = (keep_g, keep_u, keep_d)
    picked = (hot_g, hot_u, hot_d)
    cut = (cut_g, cut_g, cut_d)
    for xx in range(2):
        for t in range(N_T):
            i = xx * N_T + t
            remote(part(2 * xx + 1 - c)[t], got[t].at[xx], rs_s.at[i], rs_r.at[i], to_p).start()
    after_step()
    for xx in range(2):
        for t in range(N_T):
            landed(got[t].at[xx], rs_r.at[xx * N_T + t])

    def of_chip(xx, out):
        for h in range(hot):
            here = lax.rem(ids[h] // exp_per_ep, 2) == c
            for t in range(N_T):
                rows = pl.ds(pl.multiple_of((2 * xx + c) * cut[t], cut[t]), cut[t])
                out[t][h] = jnp.where(here, picked[t][h, rows, :], got[t][xx, h])

    of_chip(1 - x, snd)
    of_chip(x, keep)
    for t in range(N_T):
        i = 2 * N_T + t
        remote(snd[t], got_x[t], rs_s.at[i], rs_r.at[i], to_x).start()
    for t in range(N_T):
        landed(got_x[t], rs_r.at[2 * N_T + t])
    for h in range(hot):
        here = ids[h] // exp_per_ep // 2 == x
        for t in range(N_T):
            (sel_g, sel_u, sel_d)[t][h] = jnp.where(here, keep[t][h], got_x[t][h])
    sel = (sel_g, sel_u, sel_d)

    def broadcast(src, zz, k):
        dst = piece(p, e, zz)
        send(src, dst, x_s, x_r, k, to_x)
        send(src, dst, y_s, y_r, k, to_y)
        send(src, dst, p_s, p_r, k, to_p)

    mine = piece(p, e, z)
    UP, DOWN = 0, 1

    @pl.when(z < FS - 1)
    def _():
        send(sel, mine, z_s, z_r, UP * FS + 1, (z + 1, p, e))

    @pl.when(z > 0)
    def _():
        send(sel, mine, z_s, z_r, DOWN * FS + 1, (z - 1, p, e))

    broadcast(sel, z, z)
    after_step()
    for t in range(N_T):
        pltpu.make_async_copy(sel[t], mine[t], own.at[t]).start()

    def z_step(k):
        @pl.when(z - k >= 0)
        def _():
            src = piece(p, e, z - k)
            arrived(src, z_r, UP * FS + k)

            @pl.when(z < FS - 1)
            def _():
                send(src, src, z_s, z_r, UP * FS + k + 1, (z + 1, p, e))

            broadcast(src, z - k, z - k)

        @pl.when(z + k < FS)
        def _():
            src = piece(p, e, z + k)
            arrived(src, z_r, DOWN * FS + k)

            @pl.when(z > 0)
            def _():
                send(src, src, z_s, z_r, DOWN * FS + k + 1, (z - 1, p, e))

            broadcast(src, z + k, z + k)

    def plane_step(zz):
        from_x = piece(p, q_x, zz)
        arrived(from_x, x_r, zz)
        a = piece(p, q_x, zz, 0, half)
        send(a, a, da_s, da_r, zz, to_y)
        send(from_x, from_x, px_s, px_r, zz, to_p)
        from_y = piece(1 - p, e, zz)
        arrived(from_y, y_r, zz)
        b = piece(1 - p, e, zz, half, hot)
        send(b, b, db_s, db_r, zz, to_x)
        send(from_y, from_y, py_s, py_r, zz, to_p)

    def diagonal_step(zz):
        a = piece(1 - p, q_x, zz, 0, half)
        arrived(a, da_r, zz)
        send(a, a, pa_s, pa_r, zz, to_p)
        b = piece(1 - p, q_x, zz, half, hot)
        arrived(b, db_r, zz)
        send(b, b, pb_s, pb_r, zz, to_p)

    for k in range(1, FS):
        z_step(k)
        after_step()
    for k in range(FS):
        plane_step(lax.rem(z + k, FS))
        after_step()
    for k in range(FS):
        diagonal_step(lax.rem(z + k, FS))
        after_step()
    after_step()

    for t in range(N_T):
        pltpu.make_async_copy(sel[t], mine[t], own.at[t]).wait()
    for i in range(3 * N_T):
        t = i % N_T
        remote(sel[t], sel[t], rs_s.at[i], rs_s.at[i], to_p).wait_send()
    for k in range(1, FS):
        @pl.when(jnp.logical_and(z - k + 1 >= 0, z < FS - 1))
        def _():
            sent(mine, z_s, UP * FS + k, (z + 1, p, e))

        @pl.when(jnp.logical_and(z + k - 1 < FS, z > 0))
        def _():
            sent(mine, z_s, DOWN * FS + k, (z - 1, p, e))
    for zz in range(FS):
        src = piece(p, e, zz)
        sent(src, x_s, zz, to_x)
        sent(src, y_s, zz, to_y)
        sent(src, p_s, zz, to_p)
        sent(src, px_s, zz, to_p)
        sent(src, py_s, zz, to_p)
        a = piece(p, q_x, zz, 0, half)
        b = piece(p, q_x, zz, half, hot)
        sent(a, da_s, zz, to_y)
        sent(b, db_s, zz, to_x)
        sent(a, pa_s, zz, to_p)
        sent(b, pb_s, zz, to_p)
        q_px = 2 * (1 - x) + (1 - c)
        arrived(piece(p, q_p, zz), p_r, zz)
        arrived(piece(p, q_px, zz), px_r, zz)
        arrived(piece(1 - p, q_p, zz), py_r, zz)
        arrived(piece(1 - p, q_px, zz, 0, half), pa_r, zz)
        arrived(piece(1 - p, q_px, zz, half, hot), pb_r, zz)
    for t in range(N_T):
        for kk in range(FS):
            zz = lax.rem(z + kk, FS)
            if (kk, t) != (LATE, 2):
                main_sent(zz, 0, t)
                main_sent(zz, 1, t)
    pltpu.make_async_copy(late_src, late, loc.at[N_T]).wait()
    for ys in range(PP):
        for zs in range(FS):
            main_landed(ys, zs)


def exchange(ids, w_gate, w_up, w_down, hot_g, hot_u, hot_d):
    dt = w_gate.dtype
    exp_local, d, f = w_gate.shape[1:]
    hot = hot_g.shape[0]
    per_dev = exp_local // (FS * PP)
    full = f * FS
    dma = lambda n: pltpu.SemaphoreType.DMA((n,))
    quarter = [(hot, d // EP, f), (hot, d // EP, f), (hot, f // EP, d)]
    four = lambda: [dma(FS * N_T), dma(FS * N_T)]
    return pl.pallas_call(
        functools.partial(exchange_body, exp_local),
        out_shape=(
            pltpu.HBM((PP, per_dev, d, 2 * full), dt),
            pltpu.HBM((PP, per_dev, full, d), dt),
            pltpu.HBM((PP, hot, d, 2 * full), dt),
            pltpu.VMEM((PP, hot, full, d), dt),
            pltpu.HBM((per_dev, f, d), dt),
        ),
        in_specs=[pl.BlockSpec(memory_space=pltpu.SMEM)] + [HBM] * N_T + [VMEM] * N_T,
        out_specs=(HBM, HBM, HBM, VMEM, HBM),
        scratch_shapes=[pltpu.VMEM((2,) + s, dt) for s in quarter]
        + [pltpu.VMEM(s, dt) for s in quarter] * 4
        + [dma(FS * PP * N_T), dma(FS * PP * N_T), dma(EP * N_T), dma(EP * N_T), dma(N_T + 1), dma(N_T)]
        + [dma(2 * FS * N_T), dma(2 * FS * N_T)]
        + four() * 9,
        compiler_params=pltpu.CompilerParams(has_side_effects=True, vmem_limit_bytes=16 << 20),
        cost_estimate=pl.CostEstimate(flops=1 << 36, bytes_accessed=1 << 27, transcendentals=0),
        name="exchange",
    )(ids, w_gate, w_up, w_down, hot_g, hot_u, hot_d)


def place_of(piece, whole, lay):
    f = piece.shape[1]
    zz = lax.rem(lax.axis_index("fs") + LATE, FS)
    return whole.at[lay, :, pl.ds(pl.multiple_of(zz * f, f), f), :]


def settle_body(n_slot, ahead, w13, w2, hot13, hot2, early, w13_out, w2_out, hot13_out, hot2_out, buf, r_sem, w_sem, hot_sem, early_sem):
    steps = [
        (src, dst, i, j)
        for src, dst in ((w2, w2_out), (w13, w13_out), (hot13, hot13_out))
        for i in range(src.shape[0])
        for j in range(src.shape[1])
    ]
    n_first = w2.shape[0] * w2.shape[1]
    direct = [pltpu.make_async_copy(hot2.at[i], hot2_out.at[i], hot_sem.at[i]) for i in range(hot2.shape[0])]
    core = lax.rem(lax.axis_index("ep"), 2)
    early_copy = pltpu.make_async_copy(early, place_of(early, w2_out, 1 - core), early_sem)

    def load(k):
        src, dst, i, j = steps[k]
        return pltpu.make_async_copy(src.at[i, j], buf.at[k % n_slot, pl.ds(0, src.shape[2])], r_sem.at[k % n_slot])

    def store(k):
        src, dst, i, j = steps[k]
        return pltpu.make_async_copy(buf.at[k % n_slot, pl.ds(0, src.shape[2])], dst.at[i, j], w_sem.at[k % n_slot])

    for k in range(ahead):
        load(k).start()
    for copy in direct:
        copy.start()
    for k in range(len(steps)):
        load(k).wait()
        store(k).start()
        if k + ahead < len(steps):
            old = k + ahead - n_slot
            if old >= 0:
                store(old).wait()
            if old == n_first - 1:
                early_copy.start()
            load(k + ahead).start()
    for k in range(len(steps) - n_slot, len(steps)):
        store(k).wait()
    for copy in direct:
        copy.wait()
    early_copy.wait()


def settle(w13, w2, hot13, hot2, early):
    n_slot, ahead = 12, 7
    arrays = [in_hbm(w13), in_hbm(w2), in_hbm(hot13), in_vmem(hot2)]
    size = sum(a.size * a.dtype.itemsize for a in arrays)
    return pl.pallas_call(
        functools.partial(settle_body, n_slot, ahead),
        out_shape=tuple(pltpu.HBM(a.shape, a.dtype) for a in arrays),
        in_specs=[HBM, HBM, HBM, VMEM, VMEM],
        out_specs=(HBM,) * len(arrays),
        scratch_shapes=[
            pltpu.VMEM((n_slot,) + w13.shape[2:], w13.dtype),
            pltpu.SemaphoreType.DMA((n_slot,)),
            pltpu.SemaphoreType.DMA((n_slot,)),
            pltpu.SemaphoreType.DMA((PP,)),
            pltpu.SemaphoreType.DMA,
        ],
        compiler_params=pltpu.CompilerParams(vmem_limit_bytes=26 << 20),
        cost_estimate=pl.CostEstimate(flops=size * 16, bytes_accessed=2 * size, transcendentals=0),
        name="settle",
    )(*arrays, early)


def insert_body(piece, whole_in, whole_out, sem):
    copy = pltpu.make_async_copy(piece, place_of(piece, whole_out, lax.rem(lax.axis_index("ep"), 2)), sem)
    copy.start()
    copy.wait()


def insert(whole, piece):
    return pl.pallas_call(
        insert_body,
        out_shape=jax.ShapeDtypeStruct(whole.shape, whole.dtype),
        in_specs=[pl.BlockSpec(memory_space=pltpu.VMEM), HBM],
        out_specs=HBM,
        scratch_shapes=[pltpu.SemaphoreType.DMA],
        compiler_params=pltpu.CompilerParams(vmem_limit_bytes=4 << 20),
        input_output_aliases={1: 0},
        name="insert",
    )(piece, whole)


def stage_body(down, out, sem):
    z, p = lax.axis_index("fs"), lax.axis_index("pp")
    n = out.shape[0]
    copy = pltpu.make_async_copy(down.at[0, pl.ds(n * ((1 - p) * FS + lax.rem(z + LATE, FS)), n)], out, sem)
    copy.start()
    copy.wait()


def stage(w_down):
    exp_local, f, d = w_down.shape[1:]
    return pl.pallas_call(
        stage_body,
        out_shape=pltpu.VMEM((exp_local // (FS * PP), f, d), w_down.dtype),
        in_specs=[HBM],
        out_specs=VMEM,
        scratch_shapes=[pltpu.SemaphoreType.DMA],
        compiler_params=pltpu.CompilerParams(vmem_limit_bytes=4 << 20),
        name="stage",
    )(w_down)


def piece_pairs(core_of_stage):
    flat = lambda z, p, e: (z * PP + p) * EP + e
    return [
        (flat(z, p, e), flat((z + LATE) % FS, e // 2, (2 * e + core_of_stage(p)) % EP))
        for z in range(FS)
        for p in range(PP)
        for e in range(EP)
    ]


def solution(mesh):
    in_spec = P("pp", "ep", None, "fs")
    down_spec = P("pp", "ep", "fs", None)
    home_spec = P(None, ("pp", "ep", "fs"), None, None)

    def device_body(w_gate, w_up, w_down, hot_ids):
        w_gate, w_up, w_down = in_hbm(w_gate), in_hbm(w_up), in_hbm(w_down)
        early = lax.ppermute(stage(w_down), ("fs", "pp", "ep"), piece_pairs(lambda p: 1 - p))
        picked = map(in_vmem, pick(hot_ids, w_gate, w_up, w_down))
        *came, late = exchange(hot_ids, w_gate, w_up, w_down, *picked)
        late = lax.ppermute(late, ("fs", "pp", "ep"), piece_pairs(lambda p: p))
        w13, w2, hot13, hot2 = settle(*came, early)
        w2 = insert(w2, late)
        return w13, w2, hot13, hot2

    return jax.shard_map(
        device_body,
        mesh=mesh,
        in_specs=(in_spec, in_spec, down_spec, P()),
        out_specs=(home_spec, home_spec, P(), P()),
        check_vma=False,
    )
```
